32 devices in a mesh: dev: 16 (over z, y, x), rep: 2 (over core).
Axes of the slice: x: 2, y: 2, z: 4, core: 2. Of those that a mesh axis runs over, the one named last changes fastest.
Arguments:
- embeddings: float32 [4096, 4096], P(('rep', 'dev')), parts along dimension 0, may hold values from -130 to 130
- cluster_id: int32 [4096], P(('rep', 'dev')), parts along dimension 0, may hold values from 0 to 31, as said below
- member_order: int32 [4096], P(('rep', 'dev')), parts along dimension 0, may hold values from 0 to 127, as said below
- cluster_slot: int32 [64], P('rep'), parts along dimension 0, may hold values from 0 to 31, each once
- cluster_size: int32 [64], P('rep'), parts along dimension 0, may hold values from 16 to 128, as said below
Outputs:
- best_similarity: float32 [4096], P(('rep', 'dev')), parts along dimension 0
- keep: int32 [4096], P(('rep', 'dev')), parts along dimension 0
- cluster_mean: float32 [64], P(('rep', 'dev')), parts along dimension 0
The draws below stay inside these ranges and needn't reach their ends.
There are 2 independent parts, one for each index of `rep`. The reference program is written for one: setup_inputs(seed, part) draws one part's arguments, and reference() takes and returns one part's arrays. A program takes and returns all parts, laid end to end along the dimension named above; each array names one. Nothing has to cross between parts.
Inputs may be any that keep to these rules, and one draw needn't show every extreme that they name: `cluster_id`: every cluster holds at most 128 rows and some cluster exactly 128. A cluster of n members has floor(n / 16) or ceil(n / 16) of them among the rows of each device, so at most 8, a number reached on every device. `member_order`: within a cluster of n members the ranks are 0 to n - 1, each once. `cluster_slot`: a permutation; cluster c is owned by device cluster_slot[c] // 2 of dev. `cluster_size`: the number of rows whose cluster_id is c.
All inputs are finite; a program needn't handle non-finite values.
Results may differ from the reference program's by a relative error of at most 0.0003.
Values may be sent and summed in bfloat16 or wider, within the bound.
A program may use at most 64 MiB of HBM per device.

```python
import jax
import jax.numpy as jnp
from jax import lax

D = 4096
CAP = 128
CLUSTERS = 32
ROWS_ALL = 2048
N_DEV = 16


def layout(key):
    base_key = jax.random.fold_in(key, 7)
    key_sizes, key_labels, key_order, key_source, key_rows = jax.random.split(base_key, 5)
    half_count = CLUSTERS // 2
    sizes_pair = jax.random.randint(key_sizes, (half_count,), CAP // 8, CAP - CAP // 8 + 1)
    base_sizes = jnp.concatenate([sizes_pair, CAP - sizes_pair]).astype(jnp.int32)
    base_sizes = base_sizes.at[0].set(CAP).at[half_count].set(CAP // 2).at[1].set(CAP // 4).at[half_count + 1].set(CAP // 4)
    labels = jax.random.permutation(key_labels, CLUSTERS)
    sizes_out = jnp.zeros((CLUSTERS,), jnp.int32).at[labels].set(base_sizes)
    size_ends = jnp.cumsum(sizes_out)
    size_starts = size_ends - sizes_out
    positions = jnp.arange(ROWS_ALL, dtype=jnp.int32)
    owner_cluster = jnp.sum((positions[:, None] >= size_ends[None, :]).astype(jnp.int32), axis=1)
    shuffle = jax.random.permutation(key_order, ROWS_ALL).astype(jnp.int32)
    ranked = jnp.argsort(owner_cluster * ROWS_ALL + shuffle, stable=True)
    inverse = jnp.zeros((ROWS_ALL,), jnp.int32).at[ranked].set(positions)
    orders = inverse - size_starts[owner_cluster]
    source_perm = jax.random.permutation(key_source, N_DEV).astype(jnp.int32)
    source = source_perm[positions % N_DEV]
    second = jax.random.permutation(key_rows, ROWS_ALL).astype(jnp.int32)
    placed = jnp.argsort(source * ROWS_ALL + second, stable=True)
    target = jnp.zeros((ROWS_ALL,), jnp.int32).at[placed].set(positions)
    ids_out = jnp.zeros((ROWS_ALL,), jnp.int32).at[target].set(owner_cluster)
    order_out = jnp.zeros((ROWS_ALL,), jnp.int32).at[target].set(orders)
    return (ids_out, order_out, sizes_out)


def draw_cluster_id(key, part):
    return layout(key)[0]


def draw_member_order(key, part):
    return layout(key)[1]


def draw_cluster_size(key, part):
    return layout(key)[2]


def draw_embeddings(key, part):
    cluster_ids = layout(key)[0]
    base_key = jax.random.fold_in(key, 11)
    key_anchor, key_noise, key_copy = jax.random.split(base_key, 3)
    anchors = jnp.clip(jax.random.normal(key_anchor, (CLUSTERS, D), jnp.float32), -8.0, 8.0)
    noise = jnp.clip(jax.random.normal(key_noise, (ROWS_ALL, D), jnp.float32), -8.0, 8.0)
    copied = jax.random.randint(key_copy, (ROWS_ALL,), 0, 3) == 0
    values = jnp.where(copied[:, None], anchors[cluster_ids] + 0.15 * noise, noise)
    return values.astype(jnp.float32)


def setup_inputs(seed: int = 0, part: int = 0) -> dict:
    key_list = jax.random.split(jax.random.key(seed), 6)
    own_keys = jax.random.split(jax.random.fold_in(key_list[5], part), 6)
    embeddings = draw_embeddings(jax.random.fold_in(jax.random.fold_in(key_list[5], part), 71), part)
    cluster_id = draw_cluster_id(jax.random.fold_in(jax.random.fold_in(key_list[5], part), 71), part)
    member_order = draw_member_order(jax.random.fold_in(jax.random.fold_in(key_list[5], part), 71), part)
    cluster_slot = jax.random.permutation(own_keys[3], CLUSTERS).astype(jnp.int32)
    cluster_size = draw_cluster_size(jax.random.fold_in(jax.random.fold_in(key_list[5], part), 71), part)
    return {"embeddings": embeddings, "cluster_id": cluster_id, "member_order": member_order, "cluster_slot": cluster_slot, "cluster_size": cluster_size}


norm_eps = 1e-06
cutoff = 0.8

def normalized(values):
    squares_sum = lax.optimization_barrier(jnp.sum(values * values, axis=1, keepdims=True))
    return (values * lax.rsqrt(squares_sum + norm_eps)).astype(jnp.bfloat16)

def reference(embeddings, cluster_id, member_order, cluster_slot, cluster_size):
    unit_rows = normalized(embeddings)
    total_rows = embeddings.shape[0]
    where_put = (cluster_id * CAP + member_order).astype(jnp.int32)
    index_table = jnp.zeros((CLUSTERS * CAP,), jnp.int32).at[where_put].set(jnp.arange(total_rows, dtype=jnp.int32) + 1).reshape(CLUSTERS, CAP)
    spot_index = jnp.arange(CAP, dtype=jnp.int32)
    lower = spot_index[None, :] < spot_index[:, None]

    def one_cluster(packed):
        entries, size_now = packed
        occupied = entries > 0
        gathered = unit_rows[jnp.maximum(entries - 1, 0)].astype(jnp.float32)
        members = jnp.where(occupied[:, None], gathered, 0.0)
        is_live = occupied & (spot_index < size_now)
        similar = jnp.dot(members, members.T, preferred_element_type=jnp.float32)
        allowed = lower & is_live[None, :]
        nearest = lax.optimization_barrier(jnp.max(jnp.where(allowed, similar, -1.0), axis=1))
        best_spot = jnp.where(is_live, nearest, -1.0)
        mean_best = jnp.sum(jnp.where(is_live, best_spot, 0.0)) / size_now.astype(jnp.float32)
        return (best_spot, mean_best)
    best_table, cluster_means = lax.map(one_cluster, (index_table, cluster_size))
    row_best = best_table.reshape(-1)[where_put]
    keep_mask = (row_best < cutoff).astype(jnp.int32)
    by_slot = jnp.zeros((CLUSTERS,), jnp.float32).at[cluster_slot].set(cluster_means)
    return (row_best, keep_mask, by_slot)
```

```python
import functools

import jax
import jax.numpy as jnp
from jax import lax
from jax.experimental import pallas as pl
from jax.experimental.pallas import tpu as pltpu
from jax.sharding import PartitionSpec as P

CAP = 128
CHUNK = 256
NORM_EPS = 1e-06
CUTOFF = 0.8
F32 = jnp.float32
BF16 = jnp.bfloat16
I32 = jnp.int32


def split_lines(n):
    for z in range(1, n + 1):
        if n % z == 0 and z * z >= n:
            return z, n // z


def iota(shape, dim):
    return lax.broadcasted_iota(I32, shape, dim)


def rows_of(values, width):
    row = iota((8, width), 0)
    out = jnp.zeros((8, width), values[0].dtype)
    for r, v in enumerate(values):
        out = jnp.where(row == r, jnp.broadcast_to(v, (8, width)), out)
    return out


def to_col(row, count):
    eye = iota((count, count), 0) == iota((count, count), 1)
    return jnp.sum(jnp.where(eye, row, 0.0), axis=1, keepdims=True)


def floor_div(x, d):
    return jnp.floor((x + 0.5) * (1.0 / d))


def kernel(n, nz, nq, emb, cid, order, slot, size, best_out, keep_out, mean_out,
           unit, line, meta, place, pick, packed, plane, ots, otr, gram, hs, hr, table,
           s_meta, r_meta, s_line, r_line, s_plane, r_plane, s_ot, r_ot, s_h, r_h, s_t, r_t):
    me = lax.axis_index("dev")
    z, q = lax.div(me, nq), lax.rem(me, nq)
    rows = emb.shape[0]
    clusters = slot.shape[1]
    per_owner = clusters // n
    chunks, width = unit.shape[1], unit.shape[3]
    group = nz * per_owner
    seg = CAP // nq
    slots = group * seg
    half = CAP // 2

    def copy(src, dst, s, r, target):
        return pltpu.make_async_remote_copy(
            src_ref=src, dst_ref=dst, send_sem=s, recv_sem=r,
            device_id={"dev": target}, device_id_type=pl.DeviceIdType.MESH)

    def on_line(d):
        return lax.rem(z + d, nz)

    def on_plane(d):
        return lax.rem(q + d, nq)

    barrier = pltpu.get_barrier_semaphore()
    for d in range(1, n):
        pl.semaphore_signal(barrier, inc=1, device_id={"dev": lax.rem(me + d, n)},
                            device_id_type=pl.DeviceIdType.MESH)

    meta[z] = rows_of([cid[...], order[...]], rows)
    x = emb[...]
    scale = lax.rsqrt(jnp.sum(x * x, axis=1, keepdims=True) + NORM_EPS)
    pl.semaphore_wait(barrier, n - 1)

    started = []
    metas = [copy(meta.at[z], meta.at[z], s_meta.at[d], r_meta.at[d], on_line(d) * nq + q)
             for d in range(1, nz)]
    for c in metas:
        c.start()
    lines = []
    for k in range(chunks):
        for t in range(nz):
            c0 = (t * chunks + k) * width
            unit[t, k] = (emb[:, c0:c0 + width] * scale).astype(BF16)
        now = [copy(unit.at[on_line(d), k], line.at[k, z], s_line.at[k, d], r_line.at[k, d],
                    on_line(d) * nq + q) for d in range(1, nz)]
        for c in now:
            c.start()
        line[k, z] = unit[z, k]
        lines.append(now)

    slot_c = to_col(slot[...].astype(F32), clusters)
    size_c = to_col(size[...].astype(F32), clusters)
    owner_c = floor_div(slot_c, per_owner)
    local_c = slot_c - owner_c * per_owner
    oz_c = floor_div(owner_c, nq)
    oq_c = owner_c - oz_c * nq
    place_c = oq_c * slots + (oz_c * per_owner + local_c) * seg
    s8_c = owner_c * 8 + local_c
    for c in metas:
        c.wait_recv()
    tri = (iota((rows, rows), 0) < iota((rows, rows), 1)).astype(F32).astype(BF16)
    base = jnp.zeros((clusters, 1), F32)
    for b in range(nz):
        is_mem = iota((clusters, rows), 0) == meta[b, 0:1, :]
        mem = is_mem.astype(F32)
        before = base + jnp.dot(mem.astype(BF16), tri, preferred_element_type=F32)

        def of_row(v):
            return jnp.sum(jnp.where(is_mem, v, 0.0), axis=0, keepdims=True)

        rank = of_row(before)
        vals = [of_row(place_c) + rank, rank + (q * seg).astype(F32), of_row(s8_c),
                meta[b, 1:2, :].astype(F32) + 1.0]
        place[:, b * rows:(b + 1) * rows] = rows_of(vals, rows)
        base = base + jnp.sum(mem, axis=1, keepdims=True)

    all_rows = nz * rows
    place_i = place[0:1, :].astype(I32)
    key_i = (place[2:3, :] * CAP + place[1:2, :]).astype(I32)
    order_b = jnp.broadcast_to(place[3:4, :], (8, all_rows)).astype(BF16)

    def make_pick(t, _):
        hit = iota((slots, all_rows), 0) + t * slots == place_i
        pick[t] = jnp.where(hit, 1.0, 0.0).astype(BF16)
        rows_l = []
        for l in range(per_owner):
            at = ((z * nq + t) * 8 + l) * CAP
            sel = jnp.where(iota((CAP, all_rows), 0) + at == key_i, 1.0, 0.0).astype(BF16)
            r = lax.dot_general(order_b, sel, (((1,), (1,)), ((), ())), preferred_element_type=F32)
            rows_l.append(r[0:1, :])
        ots[t] = rows_of(rows_l, CAP)
        return 0

    lax.fori_loop(0, nq, make_pick, 0)
    otr[q] = ots[q]
    orders = [copy(ots.at[on_plane(d)], otr.at[q], s_ot.at[d], r_ot.at[d], z * nq + on_plane(d))
              for d in range(1, nq)]
    for c in orders:
        c.start()

    planes = []
    for k in range(chunks):
        for c in lines[k]:
            c.wait_recv()
        block = line[k].reshape(all_rows, width)
        now = []
        for d in list(range(1, nq)) + [0]:
            t = on_plane(d)
            got = jnp.dot(pick[t], block, preferred_element_type=F32).astype(BF16)
            got = got.reshape(group, seg, width)
            if d == 0:
                plane[k, q] = got
            else:
                packed[k, t] = got
                c = copy(packed.at[k, t], plane.at[k, q], s_plane.at[k, d], r_plane.at[k, d],
                         z * nq + t)
                c.start()
                now.append(c)
        planes.append(now)

    for k in range(chunks):
        for c in planes[k]:
            c.wait_recv()
        for e in range(group):
            m = plane[k, :, e].reshape(CAP, width)
            s = lax.dot_general(m, m, (((1,), (1,)), ((), ())), preferred_element_type=F32)
            if k == 0:
                gram[e] = s
            else:
                gram[e] = gram[e] + s

    below = iota((half, CAP), 0) + half > iota((half, CAP), 1)

    def pack_half(t, _):
        for l in range(per_owner):
            full = gram[t * per_owner + l]
            hs[t, l] = jnp.where(below, full[half:, :], pltpu.roll(full[:half, :], half, 1))
        return 0

    lax.fori_loop(0, nz, pack_half, 0)
    halves = [copy(hs.at[on_line(d)], hr.at[z], s_h.at[d], r_h.at[d], on_line(d) * nq + q)
              for d in range(1, nz)]
    for c in halves:
        c.start()
    hr[z] = hs[z]
    for c in orders:
        c.wait_recv()
    ord_r = otr[0]
    for t in range(1, nq):
        ord_r = ord_r + otr[t]
    ord_cols = ord_r.T
    for c in halves:
        c.wait_recv()
    bests, means = [], []
    up = iota((half, half), 0) < iota((half, half), 1)
    down = iota((half, half), 0) > iota((half, half), 1)
    for l in range(per_owner):
        p = hr[0, l]
        for t in range(1, nz):
            p = p + hr[t, l]
        pt = p.T
        u, ut = p[:, half:], pt[half:, :]
        top = jnp.concatenate([jnp.where(up, u, ut), pt[:half, :]], axis=1)
        bottom = jnp.concatenate([p[:, :half], jnp.where(down, u, ut)], axis=1)
        sim = jnp.concatenate([top, bottom], axis=0)
        mine = (me * per_owner + l).astype(F32)
        n_mem = jnp.sum(jnp.where(slot_c == mine, size_c, 0.0), axis=0, keepdims=True)
        o_row, o_col = ord_r[l:l + 1, :], ord_cols[:, l:l + 1]
        ok = (o_col < o_row) & (o_col >= 1.0) & (o_col <= n_mem)
        near = jnp.max(jnp.where(ok, sim, -1.0), axis=0, keepdims=True)
        live = (o_row >= 1.0) & (o_row <= n_mem)
        bests.append(jnp.where(live, near, -1.0))
        means.append(jnp.sum(jnp.where(live, near, 0.0), axis=1, keepdims=True) / n_mem)
    table[me] = rows_of(bests, CAP)
    backs = [copy(table.at[me], table.at[me], s_t.at[d], r_t.at[d], lax.rem(me + d, n))
             for d in range(1, n)]
    for c in backs:
        c.start()
    mean = jnp.zeros((1, per_owner), F32)
    for l in range(per_owner):
        mean = jnp.where(iota((1, per_owner), 1) == l, means[l], mean)
    mean_out[...] = mean

    own = pl.ds(pl.multiple_of(z * rows, rows), rows)
    s8 = place[2:3, own].astype(I32)
    pos = place[1:2, own].astype(I32)
    hot = jnp.where(iota((n * 8, rows), 0) == s8, 1.0, 0.0)
    for c in backs:
        c.wait_recv()
    flat = table[...].reshape(n * 8, CAP).T
    got = jnp.dot(flat, hot, preferred_element_type=F32, precision=lax.Precision.HIGHEST)
    out = jnp.sum(jnp.where(iota((CAP, rows), 0) == pos, got, 0.0), axis=0, keepdims=True)
    best_out[...] = out
    keep_out[...] = jnp.where(out < CUTOFF, 1, 0)
    for group_of in [metas, orders, halves, backs] + lines + planes:
        for c in group_of:
            c.wait_send()


def body(embeddings, cluster_id, member_order, cluster_slot, cluster_size):
    n = lax.axis_size("dev")
    nz, nq = split_lines(n)
    rows, depth = embeddings.shape
    clusters = cluster_slot.shape[0]
    per_owner = clusters // n
    width = min(CHUNK, depth // nz)
    chunks = depth // nz // width
    group, seg = nz * per_owner, CAP // nq
    vmem = pl.BlockSpec(memory_space=pltpu.VMEM)
    dma = pltpu.SemaphoreType.DMA
    best, keep, mean = pl.pallas_call(
        functools.partial(kernel, n, nz, nq),
        out_shape=(jax.ShapeDtypeStruct((1, rows), F32), jax.ShapeDtypeStruct((1, rows), I32),
                   jax.ShapeDtypeStruct((1, per_owner), F32)),
        in_specs=[vmem] * 5,
        out_specs=(vmem,) * 3,
        scratch_shapes=[
            pltpu.VMEM((nz, chunks, rows, width), BF16),
            pltpu.VMEM((chunks, nz, rows, width), BF16),
            pltpu.VMEM((nz, 8, rows), I32),
            pltpu.VMEM((8, nz * rows), F32),
            pltpu.VMEM((nq, group * seg, nz * rows), BF16),
            pltpu.VMEM((chunks, nq, group, seg, width), BF16),
            pltpu.VMEM((chunks, nq, group, seg, width), BF16),
            pltpu.VMEM((nq, 8, CAP), F32),
            pltpu.VMEM((nq, 8, CAP), F32),
            pltpu.VMEM((group, CAP, CAP), F32),
            pltpu.VMEM((nz, per_owner, CAP // 2, CAP), F32),
            pltpu.VMEM((nz, per_owner, CAP // 2, CAP), F32),
            pltpu.VMEM((n, 8, CAP), F32),
            dma((nz,)), dma((nz,)),
            dma((chunks, nz)), dma((chunks, nz)),
            dma((chunks, nq)), dma((chunks, nq)),
            dma((nq,)), dma((nq,)),
            dma((nz,)), dma((nz,)),
            dma((n,)), dma((n,)),
        ],
        compiler_params=pltpu.CompilerParams(
            collective_id=0, has_side_effects=True, vmem_limit_bytes=60 * 1024 * 1024),
    )(embeddings, cluster_id.reshape(1, rows), member_order.reshape(1, rows),
      cluster_slot.reshape(1, clusters), cluster_size.reshape(1, clusters))
    return best.reshape(rows), keep.reshape(rows), mean.reshape(per_owner)


def solution(mesh):
    placed = (P(("rep", "dev"), None), P(("rep", "dev")), P(("rep", "dev")), P("rep"), P("rep"))
    return jax.shard_map(
        body,
        mesh=mesh,
        in_specs=placed,
        out_specs=(P(("rep", "dev")), P(("rep", "dev")), P(("rep", "dev"))),
        check_vma=False,
    )
```

```python
import functools

import jax
import jax.numpy as jnp
from jax import lax
from jax.experimental import pallas as pl
from jax.experimental.pallas import tpu as pltpu
from jax.sharding import PartitionSpec as P

CAP = 128
CHUNK = 128
LOADS = 4
LAG = 2
NORM_EPS = 1e-06
CUTOFF = 0.8
F32 = jnp.float32
BF16 = jnp.bfloat16
I32 = jnp.int32


def split_lines(n):
    for z in range(1, n + 1):
        if n % z == 0 and z * z >= n:
            return z, n // z


def iota(shape, dim):
    return lax.broadcasted_iota(I32, shape, dim)


def rows_of(values, width):
    row = iota((8, width), 0)
    out = jnp.zeros((8, width), values[0].dtype)
    for r, v in enumerate(values):
        out = jnp.where(row == r, jnp.broadcast_to(v, (8, width)), out)
    return out


def to_col(row, count):
    eye = iota((count, count), 0) == iota((count, count), 1)
    return jnp.sum(jnp.where(eye, row, 0.0), axis=1, keepdims=True)


def floor_div(x, d):
    return jnp.floor((x + 0.5) * (1.0 / d))


def kernel(n, nz, nq, emb_hbm, cid, order, slot, size, packed_out,
           emb, s_load, unit, line, meta, place, pick, packed, plane, ots, otr, gram, hs, hr, table,
           s_meta, r_meta, s_line, r_line, s_plane, r_plane, s_ot, r_ot, s_h, r_h, s_t, r_t):
    me = lax.axis_index("dev")
    parts = s_load.shape[0]
    tall = emb.shape[0] // parts
    loads = [pltpu.make_async_copy(emb_hbm.at[pl.ds(i * tall, tall)], emb.at[pl.ds(i * tall, tall)],
                                   s_load.at[i]) for i in range(parts)]
    for c in loads:
        c.start()
    z, q = lax.div(me, nq), lax.rem(me, nq)
    rows = emb.shape[0]
    clusters = slot.shape[1]
    per_owner = clusters // n
    chunks, width = unit.shape[1], unit.shape[3]
    group = nz * per_owner
    seg = CAP // nq
    slots = group * seg
    half = CAP // 2

    def copy(src, dst, s, r, target):
        return pltpu.make_async_remote_copy(
            src_ref=src, dst_ref=dst, send_sem=s, recv_sem=r,
            device_id={"dev": target}, device_id_type=pl.DeviceIdType.MESH)

    def on_line(d):
        return lax.rem(z + d, nz)

    def on_plane(d):
        return lax.rem(q + d, nq)

    barrier = pltpu.get_barrier_semaphore()
    for d in range(1, n):
        pl.semaphore_signal(barrier, inc=1, device_id={"dev": lax.rem(me + d, n)},
                            device_id_type=pl.DeviceIdType.MESH)

    meta[z] = rows_of([cid[...], order[...]], rows)
    sums = []
    for i in range(parts):
        loads[i].wait()
        x = emb[i * tall:(i + 1) * tall, :]
        sums.append(jnp.sum(x * x, axis=1, keepdims=True))
    scale = lax.rsqrt(jnp.concatenate(sums, axis=0) + NORM_EPS)
    pl.semaphore_wait(barrier, n - 1)

    metas = [copy(meta.at[z], meta.at[z], s_meta.at[d], r_meta.at[d], on_line(d) * nq + q)
             for d in range(1, nz)]
    for c in metas:
        c.start()
    lines = []
    for k in range(chunks):
        for t in range(nz):
            c0 = (t * chunks + k) * width
            unit[t, k] = (emb[:, c0:c0 + width] * scale).astype(BF16)
        now = [copy(unit.at[on_line(d), k], line.at[k, z], s_line.at[k, d], r_line.at[k, d],
                    on_line(d) * nq + q) for d in range(nz - 1, 0, -1)]
        for c in now:
            c.start()
        line[k, z] = unit[z, k]
        lines.append(now)

    slot_c = to_col(slot[...].astype(F32), clusters)
    size_c = to_col(size[...].astype(F32), clusters)
    owner_c = floor_div(slot_c, per_owner)
    local_c = slot_c - owner_c * per_owner
    oz_c = floor_div(owner_c, nq)
    oq_c = owner_c - oz_c * nq
    place_c = oq_c * slots + (oz_c * per_owner + local_c) * seg
    s8_c = slot_c
    for c in metas:
        c.wait_recv()
    tri = (iota((rows, rows), 0) < iota((rows, rows), 1)).astype(F32).astype(BF16)
    base = jnp.zeros((clusters, 1), F32)
    for b in range(nz):
        is_mem = iota((clusters, rows), 0) == meta[b, 0:1, :]
        mem = is_mem.astype(F32)
        before = base + jnp.dot(mem.astype(BF16), tri, preferred_element_type=F32)

        def of_row(v):
            return jnp.sum(jnp.where(is_mem, v, 0.0), axis=0, keepdims=True)

        rank = of_row(before)
        vals = [of_row(place_c) + rank, rank + (q * seg).astype(F32), of_row(s8_c),
                meta[b, 1:2, :].astype(F32) + 1.0]
        place[:, b * rows:(b + 1) * rows] = rows_of(vals, rows)
        base = base + jnp.sum(mem, axis=1, keepdims=True)

    all_rows = nz * rows
    place_i = place[0:1, :].astype(I32)
    key_i = (place[2:3, :] * CAP + place[1:2, :]).astype(I32)
    order_b = jnp.broadcast_to(place[3:4, :], (8, all_rows)).astype(BF16)

    def make_pick(t, _):
        hit = iota((slots, all_rows), 0) + t * slots == place_i
        pick[t] = jnp.where(hit, 1.0, 0.0).astype(BF16)
        rows_l = []
        for l in range(per_owner):
            at = ((z * nq + t) * per_owner + l) * CAP
            sel = jnp.where(iota((CAP, all_rows), 0) + at == key_i, 1.0, 0.0).astype(BF16)
            r = lax.dot_general(order_b, sel, (((1,), (1,)), ((), ())), preferred_element_type=F32)
            rows_l.append(r[0:1, :])
        ots[t] = rows_of(rows_l, CAP)
        return 0

    lax.fori_loop(0, nq, make_pick, 0)
    otr[q] = ots[q]
    orders = [copy(ots.at[on_plane(d)], otr.at[q], s_ot.at[d], r_ot.at[d], z * nq + on_plane(d))
              for d in range(1, nq)]
    for c in orders:
        c.start()

    below = iota((half, CAP), 0) + half > iota((half, CAP), 1)

    def partial_gram(k, e):
        m = plane[k, :, e].reshape(CAP, width)
        return lax.dot_general(m, m, (((1,), (1,)), ((), ())), preferred_element_type=F32)

    def add_gram(k):
        for c in planes[k]:
            c.wait_recv()
        for e in range(group):
            s = partial_gram(k, e)
            gram[e] = s if k == 0 else gram[e] + s

    planes = []
    for k in range(chunks):
        for c in lines[k]:
            c.wait_recv()
        block = line[k].reshape(all_rows, width)
        now = []
        for d in list(range(1, nq)) + [0]:
            t = on_plane(d)
            got = jnp.dot(pick[t], block, preferred_element_type=F32).astype(BF16)
            got = got.reshape(group, seg, width)
            if d == 0:
                plane[k, q] = got
            else:
                packed[k, t] = got
                c = copy(packed.at[k, t], plane.at[k, q], s_plane.at[k, d], r_plane.at[k, d],
                         z * nq + t)
                c.start()
                now.append(c)
        planes.append(now)
        if k >= LAG:
            add_gram(k - LAG)

    for k in range(max(chunks - LAG, 0), chunks - 1):
        add_gram(k)
    for c in planes[chunks - 1]:
        c.wait_recv()
    halves = []
    for d in list(range(1, nz)) + [0]:
        t = on_line(d)
        for l in range(per_owner):
            full = partial_gram(chunks - 1, t * per_owner + l)
            if chunks > 1:
                full = full + gram[t * per_owner + l]
            hs[t, l] = jnp.where(below, full[half:, :], pltpu.roll(full[:half, :], half, 1))
        if d:
            c = copy(hs.at[t], hr.at[z], s_h.at[d], r_h.at[d], t * nq + q)
            c.start()
            halves.append(c)
    hr[z] = hs[z]
    for c in orders:
        c.wait_recv()
    ord_r = otr[0]
    for t in range(1, nq):
        ord_r = ord_r + otr[t]
    ord_cols = ord_r.T
    for c in halves:
        c.wait_recv()
    bests, means = [], []
    up = iota((half, half), 0) < iota((half, half), 1)
    down = iota((half, half), 0) > iota((half, half), 1)
    for l in range(per_owner):
        p = hr[0, l]
        for t in range(1, nz):
            p = p + hr[t, l]
        pt = p.T
        u, ut = p[:, half:], pt[half:, :]
        top = jnp.concatenate([jnp.where(up, u, ut), pt[:half, :]], axis=1)
        bottom = jnp.concatenate([p[:, :half], jnp.where(down, u, ut)], axis=1)
        sim = jnp.concatenate([top, bottom], axis=0)
        mine = (me * per_owner + l).astype(F32)
        n_mem = jnp.sum(jnp.where(slot_c == mine, size_c, 0.0), axis=0, keepdims=True)
        o_row, o_col = ord_r[l:l + 1, :], ord_cols[:, l:l + 1]
        ok = (o_col < o_row) & (o_col >= 1.0) & (o_col <= n_mem)
        near = jnp.max(jnp.where(ok, sim, -1.0), axis=0, keepdims=True)
        live = (o_row >= 1.0) & (o_row <= n_mem)
        bests.append(jnp.where(live, near, -1.0))
        means.append(jnp.sum(jnp.where(live, near, 0.0), axis=1, keepdims=True) / n_mem)
    table[me] = jnp.concatenate(bests, axis=0)
    backs = [copy(table.at[me], table.at[me], s_t.at[d], r_t.at[d], lax.rem(me + d, n))
             for d in range(1, n)]
    for c in backs:
        c.start()
    mean = jnp.zeros((1, rows), F32)
    for l in range(per_owner):
        mean = jnp.where(iota((1, rows), 1) == l, means[l], mean)

    own = pl.ds(pl.multiple_of(z * rows, rows), rows)
    s8 = place[2:3, own].astype(I32)
    pos = place[1:2, own].astype(I32)
    hot = jnp.where(iota((clusters, rows), 0) == s8, 1.0, 0.0)
    for c in backs:
        c.wait_recv()
    flat = table[...].reshape(clusters, CAP).T
    got = jnp.dot(flat, hot, preferred_element_type=F32, precision=lax.Precision.HIGHEST)
    out = jnp.sum(jnp.where(iota((CAP, rows), 0) == pos, got, 0.0), axis=0, keepdims=True)
    packed_out[...] = rows_of([out, mean], rows)
    for group_of in [metas, orders, halves, backs] + lines + planes:
        for c in group_of:
            c.wait_send()


def finish(packed, best_out, keep_out, mean_out):
    best = packed[0:1, :]
    best_out[...] = best
    keep_out[...] = jnp.where(best < CUTOFF, 1, 0)
    mean_out[...] = packed[1:2, :mean_out.shape[1]]


def body(embeddings, cluster_id, member_order, cluster_slot, cluster_size):
    n = lax.axis_size("dev")
    nz, nq = split_lines(n)
    rows, depth = embeddings.shape
    clusters = cluster_slot.shape[0]
    per_owner = clusters // n
    width = min(CHUNK, depth // nz)
    chunks = depth // nz // width
    group, seg = nz * per_owner, CAP // nq
    vmem = pl.BlockSpec(memory_space=pltpu.VMEM)
    dma = pltpu.SemaphoreType.DMA
    packed = pl.pallas_call(
        functools.partial(kernel, n, nz, nq),
        out_shape=jax.ShapeDtypeStruct((8, rows), F32),
        in_specs=[pl.BlockSpec(memory_space=pl.ANY)] + [vmem] * 4,
        out_specs=vmem,
        scratch_shapes=[
            pltpu.VMEM((rows, depth), F32),
            dma((LOADS,)),
            pltpu.VMEM((nz, chunks, rows, width), BF16),
            pltpu.VMEM((chunks, nz, rows, width), BF16),
            pltpu.VMEM((nz, 8, rows), I32),
            pltpu.VMEM((8, nz * rows), F32),
            pltpu.VMEM((nq, group * seg, nz * rows), BF16),
            pltpu.VMEM((chunks, nq, group, seg, width), BF16),
            pltpu.VMEM((chunks, nq, group, seg, width), BF16),
            pltpu.VMEM((nq, 8, CAP), F32),
            pltpu.VMEM((nq, 8, CAP), F32),
            pltpu.VMEM((group, CAP, CAP), F32),
            pltpu.VMEM((nz, per_owner, CAP // 2, CAP), F32),
            pltpu.VMEM((nz, per_owner, CAP // 2, CAP), F32),
            pltpu.VMEM((n, per_owner, CAP), F32),
            dma((nz,)), dma((nz,)),
            dma((chunks, nz)), dma((chunks, nz)),
            dma((chunks, nq)), dma((chunks, nq)),
            dma((nq,)), dma((nq,)),
            dma((nz,)), dma((nz,)),
            dma((n,)), dma((n,)),
        ],
        compiler_params=pltpu.CompilerParams(
            collective_id=0, has_side_effects=True, vmem_limit_bytes=60 * 1024 * 1024),
    )(embeddings, cluster_id.reshape(1, rows), member_order.reshape(1, rows),
      cluster_slot.reshape(1, clusters), cluster_size.reshape(1, clusters))
    best, keep, mean = pl.pallas_call(
        finish,
        out_shape=(jax.ShapeDtypeStruct((1, rows), F32), jax.ShapeDtypeStruct((1, rows), I32),
                   jax.ShapeDtypeStruct((1, per_owner), F32)),
        in_specs=[vmem],
        out_specs=(vmem,) * 3,
    )(packed)
    return best.reshape(rows), keep.reshape(rows), mean.reshape(per_owner)


def solution(mesh):
    placed = (P(("rep", "dev"), None), P(("rep", "dev")), P(("rep", "dev")), P("rep"), P("rep"))
    return jax.shard_map(
        body,
        mesh=mesh,
        in_specs=placed,
        out_specs=(P(("rep", "dev")), P(("rep", "dev")), P(("rep", "dev"))),
        check_vma=False,
    )
```

```python
import functools

import jax
import jax.numpy as jnp
from jax import lax
from jax.experimental import pallas as pl
from jax.experimental.pallas import tpu as pltpu
from jax.sharding import PartitionSpec as P

CAP = 128
CHUNK = 128
LOADS = 4
LAG = 2
NORM_EPS = 1e-06
CUTOFF = 0.8
F32 = jnp.float32
BF16 = jnp.bfloat16
I32 = jnp.int32


def split_lines(n):
    for z in range(1, n + 1):
        if n % z == 0 and z * z >= n:
            return z, n // z


def iota(shape, dim):
    return lax.broadcasted_iota(I32, shape, dim)


def rows_of(values, width):
    row = iota((8, width), 0)
    out = jnp.zeros((8, width), values[0].dtype)
    for r, v in enumerate(values):
        out = jnp.where(row == r, jnp.broadcast_to(v, (8, width)), out)
    return out


def to_col(row, count):
    eye = iota((count, count), 0) == iota((count, count), 1)
    return jnp.sum(jnp.where(eye, row, 0.0), axis=1, keepdims=True)


def floor_div(x, d):
    return jnp.floor((x + 0.5) * (1.0 / d))


def kernel(n, nz, nq, emb_hbm, cid, order, slot, size, packed_out,
           emb, s_load, unit, line, meta, place, pick, packed, plane, ots, otr, gram, hs, hr, table,
           s_meta, r_meta, s_line, r_line, s_plane, r_plane, s_ot, r_ot, s_h, r_h, s_t, r_t):
    me = lax.axis_index("dev")
    parts = s_load.shape[0]
    tall = emb.shape[0] // parts
    loads = [pltpu.make_async_copy(emb_hbm.at[pl.ds(i * tall, tall)], emb.at[pl.ds(i * tall, tall)],
                                   s_load.at[i]) for i in range(parts)]
    for c in loads:
        c.start()
    z, q = lax.div(me, nq), lax.rem(me, nq)
    rows = emb.shape[0]
    clusters = slot.shape[1]
    per_owner = clusters // n
    chunks, width = unit.shape[1], unit.shape[3]
    group = nz * per_owner
    seg = CAP // nq
    slots = group * seg
    half = CAP // 2

    def copy(src, dst, s, r, target):
        return pltpu.make_async_remote_copy(
            src_ref=src, dst_ref=dst, send_sem=s, recv_sem=r,
            device_id={"dev": target}, device_id_type=pl.DeviceIdType.MESH)

    def on_line(d):
        return lax.rem(z + d, nz)

    def on_plane(d):
        return lax.rem(q + d, nq)

    barrier = pltpu.get_barrier_semaphore()
    friends = [on_line(d) * nq + q for d in range(1, nz)] + [z * nq + on_plane(d) for d in range(1, nq)]
    for t in friends:
        pl.semaphore_signal(barrier, inc=1, device_id={"dev": t},
                            device_id_type=pl.DeviceIdType.MESH)

    meta[z] = rows_of([cid[...], order[...]], rows)
    sums = []
    for i in range(parts):
        loads[i].wait()
        x = emb[i * tall:(i + 1) * tall, :]
        sums.append(jnp.sum(x * x, axis=1, keepdims=True))
    scale = lax.rsqrt(jnp.concatenate(sums, axis=0) + NORM_EPS)
    pl.semaphore_wait(barrier, len(friends))

    metas = [copy(meta.at[z], meta.at[z], s_meta.at[d], r_meta.at[d], on_line(d) * nq + q)
             for d in range(1, nz)]
    for c in metas:
        c.start()
    lines = []
    for k in range(chunks):
        for t in range(nz):
            c0 = (t * chunks + k) * width
            unit[t, k] = (emb[:, c0:c0 + width] * scale).astype(BF16)
        now = [copy(unit.at[on_line(d), k], line.at[k, z], s_line.at[k, d], r_line.at[k, d],
                    on_line(d) * nq + q) for d in range(nz - 1, 0, -1)]
        for c in now:
            c.start()
        line[k, z] = unit[z, k]
        lines.append(now)

    slot_c = to_col(slot[...].astype(F32), clusters)
    size_c = to_col(size[...].astype(F32), clusters)
    owner_c = floor_div(slot_c, per_owner)
    local_c = slot_c - owner_c * per_owner
    oz_c = floor_div(owner_c, nq)
    oq_c = owner_c - oz_c * nq
    place_c = oq_c * slots + (oz_c * per_owner + local_c) * seg
    s8_c = slot_c
    for c in metas:
        c.wait_recv()
    tri = (iota((rows, rows), 0) < iota((rows, rows), 1)).astype(F32).astype(BF16)
    base = jnp.zeros((clusters, 1), F32)
    for b in range(nz):
        is_mem = iota((clusters, rows), 0) == meta[b, 0:1, :]
        mem = is_mem.astype(F32)
        before = base + jnp.dot(mem.astype(BF16), tri, preferred_element_type=F32)

        def of_row(v):
            return jnp.sum(jnp.where(is_mem, v, 0.0), axis=0, keepdims=True)

        rank = of_row(before)
        vals = [of_row(place_c) + rank, rank + (q * seg).astype(F32), of_row(s8_c),
                meta[b, 1:2, :].astype(F32) + 1.0]
        place[:, b * rows:(b + 1) * rows] = rows_of(vals, rows)
        base = base + jnp.sum(mem, axis=1, keepdims=True)

    all_rows = nz * rows
    place_i = place[0:1, :].astype(I32)
    key_i = (place[2:3, :] * CAP + place[1:2, :]).astype(I32)
    order_b = jnp.broadcast_to(place[3:4, :], (8, all_rows)).astype(BF16)

    def make_pick(t, _):
        hit = iota((slots, all_rows), 0) + t * slots == place_i
        pick[t] = jnp.where(hit, 1.0, 0.0).astype(BF16)
        rows_l = []
        for l in range(per_owner):
            at = ((z * nq + t) * per_owner + l) * CAP
            sel = jnp.where(iota((CAP, all_rows), 0) + at == key_i, 1.0, 0.0).astype(BF16)
            r = lax.dot_general(order_b, sel, (((1,), (1,)), ((), ())), preferred_element_type=F32)
            rows_l.append(r[0:1, :])
        ots[t] = rows_of(rows_l, CAP)
        return 0

    lax.fori_loop(0, nq, make_pick, 0)
    otr[q] = ots[q]
    orders = [copy(ots.at[on_plane(d)], otr.at[q], s_ot.at[d], r_ot.at[d], z * nq + on_plane(d))
              for d in range(1, nq)]
    for c in orders:
        c.start()

    below = iota((half, CAP), 0) + half > iota((half, CAP), 1)

    def partial_gram(k, e):
        m = plane[k, :, e].reshape(CAP, width)
        return lax.dot_general(m, m, (((1,), (1,)), ((), ())), preferred_element_type=F32)

    def add_gram(k):
        for c in planes[k]:
            c.wait_recv()
        for e in range(group):
            s = partial_gram(k, e)
            gram[e] = s if k == 0 else gram[e] + s

    planes = []
    for k in range(chunks):
        for c in lines[k]:
            c.wait_recv()
        block = line[k].reshape(all_rows, width)
        now = []
        for d in list(range(1, nq)) + [0]:
            t = on_plane(d)
            got = jnp.dot(pick[t], block, preferred_element_type=F32).astype(BF16)
            got = got.reshape(group, seg, width)
            if d == 0:
                plane[k, q] = got
            else:
                packed[k, t] = got
                c = copy(packed.at[k, t], plane.at[k, q], s_plane.at[k, d], r_plane.at[k, d],
                         z * nq + t)
                c.start()
                now.append(c)
        planes.append(now)
        if k >= LAG:
            add_gram(k - LAG)

    for k in range(max(chunks - LAG, 0), chunks - 1):
        add_gram(k)
    for c in planes[chunks - 1]:
        c.wait_recv()
    halves = []
    for d in list(range(1, nz)) + [0]:
        t = on_line(d)
        for l in range(per_owner):
            full = partial_gram(chunks - 1, t * per_owner + l)
            if chunks > 1:
                full = full + gram[t * per_owner + l]
            hs[t, l] = jnp.where(below, full[half:, :], pltpu.roll(full[:half, :], half, 1))
        if d:
            c = copy(hs.at[t], hr.at[z], s_h.at[d], r_h.at[d], t * nq + q)
            c.start()
            halves.append(c)
    hr[z] = hs[z]
    for c in orders:
        c.wait_recv()
    ord_r = otr[0]
    for t in range(1, nq):
        ord_r = ord_r + otr[t]
    ord_cols = ord_r.T
    for c in halves:
        c.wait_recv()
    bests, means = [], []
    up = iota((half, half), 0) < iota((half, half), 1)
    down = iota((half, half), 0) > iota((half, half), 1)
    for l in range(per_owner):
        p = hr[0, l]
        for t in range(1, nz):
            p = p + hr[t, l]
        pt = p.T
        u, ut = p[:, half:], pt[half:, :]
        top = jnp.concatenate([jnp.where(up, u, ut), pt[:half, :]], axis=1)
        bottom = jnp.concatenate([p[:, :half], jnp.where(down, u, ut)], axis=1)
        sim = jnp.concatenate([top, bottom], axis=0)
        mine = (me * per_owner + l).astype(F32)
        n_mem = jnp.sum(jnp.where(slot_c == mine, size_c, 0.0), axis=0, keepdims=True)
        o_row, o_col = ord_r[l:l + 1, :], ord_cols[:, l:l + 1]
        ok = (o_col < o_row) & (o_col >= 1.0) & (o_col <= n_mem)
        near = jnp.max(jnp.where(ok, sim, -1.0), axis=0, keepdims=True)
        live = (o_row >= 1.0) & (o_row <= n_mem)
        bests.append(jnp.where(live, near, -1.0))
        means.append(jnp.sum(jnp.where(live, near, 0.0), axis=1, keepdims=True) / n_mem)
    table[me] = jnp.concatenate(bests, axis=0)
    backs = [copy(table.at[me], table.at[me], s_t.at[d], r_t.at[d], lax.rem(me + d, n))
             for d in range(1, n)]
    for c in backs:
        c.start()
    mean = jnp.zeros((1, rows), F32)
    for l in range(per_owner):
        mean = jnp.where(iota((1, rows), 1) == l, means[l], mean)

    own = pl.ds(pl.multiple_of(z * rows, rows), rows)
    s8 = place[2:3, own].astype(I32)
    pos = place[1:2, own].astype(I32)
    hot = jnp.where(iota((clusters, rows), 0) == s8, 1.0, 0.0)
    for c in backs:
        c.wait_recv()
    flat = table[...].reshape(clusters, CAP).T
    got = jnp.dot(flat, hot, preferred_element_type=F32, precision=lax.Precision.HIGHEST)
    out = jnp.sum(jnp.where(iota((CAP, rows), 0) == pos, got, 0.0), axis=0, keepdims=True)
    packed_out[...] = rows_of([out, mean], rows)
    for group_of in [metas, orders, halves, backs] + lines + planes:
        for c in group_of:
            c.wait_send()


def finish(packed, best_out, keep_out, mean_out):
    best = packed[0:1, :]
    best_out[...] = best
    keep_out[...] = jnp.where(best < CUTOFF, 1, 0)
    mean_out[...] = packed[1:2, :mean_out.shape[1]]


def body(embeddings, cluster_id, member_order, cluster_slot, cluster_size):
    n = lax.axis_size("dev")
    nz, nq = split_lines(n)
    rows, depth = embeddings.shape
    clusters = cluster_slot.shape[0]
    per_owner = clusters // n
    width = min(CHUNK, depth // nz)
    chunks = depth // nz // width
    group, seg = nz * per_owner, CAP // nq
    vmem = pl.BlockSpec(memory_space=pltpu.VMEM)
    dma = pltpu.SemaphoreType.DMA
    packed = pl.pallas_call(
        functools.partial(kernel, n, nz, nq),
        out_shape=jax.ShapeDtypeStruct((8, rows), F32),
        in_specs=[pl.BlockSpec(memory_space=pl.ANY)] + [vmem] * 4,
        out_specs=vmem,
        scratch_shapes=[
            pltpu.VMEM((rows, depth), F32),
            dma((LOADS,)),
            pltpu.VMEM((nz, chunks, rows, width), BF16),
            pltpu.VMEM((chunks, nz, rows, width), BF16),
            pltpu.VMEM((nz, 8, rows), I32),
            pltpu.VMEM((8, nz * rows), F32),
            pltpu.VMEM((nq, group * seg, nz * rows), BF16),
            pltpu.VMEM((chunks, nq, group, seg, width), BF16),
            pltpu.VMEM((chunks, nq, group, seg, width), BF16),
            pltpu.VMEM((nq, 8, CAP), F32),
            pltpu.VMEM((nq, 8, CAP), F32),
            pltpu.VMEM((group, CAP, CAP), F32),
            pltpu.VMEM((nz, per_owner, CAP // 2, CAP), F32),
            pltpu.VMEM((nz, per_owner, CAP // 2, CAP), F32),
            pltpu.VMEM((n, per_owner, CAP), F32),
            dma((nz,)), dma((nz,)),
            dma((chunks, nz)), dma((chunks, nz)),
            dma((chunks, nq)), dma((chunks, nq)),
            dma((nq,)), dma((nq,)),
            dma((nz,)), dma((nz,)),
            dma((n,)), dma((n,)),
        ],
        compiler_params=pltpu.CompilerParams(
            collective_id=0, has_side_effects=True, vmem_limit_bytes=60 * 1024 * 1024),
    )(embeddings, cluster_id.reshape(1, rows), member_order.reshape(1, rows),
      cluster_slot.reshape(1, clusters), cluster_size.reshape(1, clusters))
    best, keep, mean = pl.pallas_call(
        finish,
        out_shape=(jax.ShapeDtypeStruct((1, rows), F32), jax.ShapeDtypeStruct((1, rows), I32),
                   jax.ShapeDtypeStruct((1, per_owner), F32)),
        in_specs=[vmem],
        out_specs=(vmem,) * 3,
    )(packed)
    return best.reshape(rows), keep.reshape(rows), mean.reshape(per_owner)


def solution(mesh):
    placed = (P(("rep", "dev"), None), P(("rep", "dev")), P(("rep", "dev")), P("rep"), P("rep"))
    return jax.shard_map(
        body,
        mesh=mesh,
        in_specs=placed,
        out_specs=(P(("rep", "dev")), P(("rep", "dev")), P(("rep", "dev"))),
        check_vma=False,
    )
```

```python
import functools

import jax
import jax.numpy as jnp
from jax import lax
from jax.experimental import pallas as pl
from jax.experimental.pallas import tpu as pltpu
from jax.sharding import PartitionSpec as P

CAP = 128
CHUNK = 128
LOADS = 4
LAG = 2
NORM_EPS = 1e-06
CUTOFF = 0.8
F32 = jnp.float32
BF16 = jnp.bfloat16
I32 = jnp.int32


def split_lines(n):
    z = max(z for z in range(1, n + 1) if n % z == 0 and z * z <= n)
    return z, n // z


def line_slots(n, nz, nq, rows, group):
    largest = rows * n // nq + CAP - CAP // nq
    bound = -(-largest // nq) + -(-group * nz * (n - 1) // n)
    return min(group * (CAP // nq), -(-bound // 16) * 16)


def iota(shape, dim):
    return lax.broadcasted_iota(I32, shape, dim)


def rows_of(values, width):
    row = iota((8, width), 0)
    out = jnp.zeros((8, width), values[0].dtype)
    for r, v in enumerate(values):
        out = jnp.where(row == r, jnp.broadcast_to(v, (8, width)), out)
    return out


def to_col(row, count):
    eye = iota((count, count), 0) == iota((count, count), 1)
    return jnp.sum(jnp.where(eye, row, 0.0), axis=1, keepdims=True)


def floor_div(x, d):
    return jnp.floor((x + 0.5) * (1.0 / d))


def kernel(n, nz, nq, emb_hbm, cid, order, slot, size, packed_out,
           emb, s_load, unit, line, meta, place, pick, packed, plane, ots, otr, gram, hs, hr, table, units, repack, labs,
           s_meta, r_meta, s_line, r_line, s_plane, r_plane, s_ot, r_ot, s_h, r_h, s_t, r_t):
    me = lax.axis_index("dev")
    parts = s_load.shape[0]
    tall = emb.shape[0] // parts
    loads = [pltpu.make_async_copy(emb_hbm.at[pl.ds(i * tall, tall)], emb.at[pl.ds(i * tall, tall)],
                                   s_load.at[i]) for i in range(parts)]
    for c in loads:
        c.start()
    z, q = lax.div(me, nq), lax.rem(me, nq)
    rows = emb.shape[0]
    clusters = slot.shape[1]
    per_owner = clusters // n
    chunks, width = unit.shape[1], unit.shape[3]
    group = nz * per_owner
    seg = CAP // nq
    slots = pick.shape[1]
    half = CAP // 2

    def copy(src, dst, s, r, target):
        return pltpu.make_async_remote_copy(
            src_ref=src, dst_ref=dst, send_sem=s, recv_sem=r,
            device_id={"dev": target}, device_id_type=pl.DeviceIdType.MESH)

    def on_line(d):
        return lax.rem(z + d, nz)

    def on_plane(d):
        return lax.rem(q + d, nq)

    barrier = pltpu.get_barrier_semaphore()
    friends = [on_line(d) * nq + q for d in range(1, nz)] + [z * nq + on_plane(d) for d in range(1, nq)]
    for t in friends:
        pl.semaphore_signal(barrier, inc=1, device_id={"dev": t},
                            device_id_type=pl.DeviceIdType.MESH)

    meta[z] = rows_of([cid[...], order[...]], rows)
    sums = []
    for i in range(parts):
        loads[i].wait()
        x = emb[i * tall:(i + 1) * tall, :]
        sums.append(jnp.sum(x * x, axis=1, keepdims=True))
    scale = lax.rsqrt(jnp.concatenate(sums, axis=0) + NORM_EPS)
    pl.semaphore_wait(barrier, len(friends))

    metas = [copy(meta.at[z], meta.at[z], s_meta.at[d], r_meta.at[d], on_line(d) * nq + q)
             for d in range(1, nz)]
    for c in metas:
        c.start()
    lines = []
    for k in range(chunks):
        for t in range(nz):
            c0 = (t * chunks + k) * width
            unit[t, k] = (emb[:, c0:c0 + width] * scale).astype(BF16)
        now = [copy(unit.at[on_line(d), k], line.at[k, z], s_line.at[k, d], r_line.at[k, d],
                    on_line(d) * nq + q) for d in range(nz - 1, 0, -1)]
        for c in now:
            c.start()
        line[k, z] = unit[z, k]
        lines.append(now)

    slot_c = to_col(slot[...].astype(F32), clusters)
    size_c = to_col(size[...].astype(F32), clusters)
    size_r = size[...].astype(F32)
    c_row, c_col = iota((clusters, clusters), 1), iota((clusters, clusters), 0)
    ahead = (size_r > size_c) | ((size_r == size_c) & (c_row < c_col))
    place_in = jnp.sum(jnp.where(ahead, 1.0, 0.0), axis=1, keepdims=True)
    e_c = floor_div(place_in, nq)
    turn = place_in - e_c * nq
    odd = e_c - 2.0 * floor_div(e_c, 2)
    g_c = jnp.where(odd > 0.5, nq - 1 - turn, turn)
    oz_c = floor_div(e_c, per_owner)
    local_c = e_c - oz_c * per_owner
    work_c = (oz_c * nq + g_c) * per_owner + local_c
    for c in metas:
        c.wait_recv()
    tri = (iota((rows, rows), 0) < iota((rows, rows), 1)).astype(F32).astype(BF16)
    counts = jnp.zeros((clusters, 1), F32)
    for b in range(nz):
        mem = jnp.where(iota((clusters, rows), 0) == meta[b, 0:1, :], 1.0, 0.0)
        counts = counts + jnp.sum(mem, axis=1, keepdims=True)
    eye = c_row == c_col
    g_r = jnp.sum(jnp.where(eye, g_c, 0.0), axis=0, keepdims=True)
    e_r = jnp.sum(jnp.where(eye, e_c, 0.0), axis=0, keepdims=True)
    n_r = jnp.sum(jnp.where(eye, counts, 0.0), axis=0, keepdims=True)
    first = (g_r == g_c) & (e_r < e_c)
    place_c = g_c * slots + jnp.sum(jnp.where(first, n_r, 0.0), axis=1, keepdims=True)
    base = jnp.zeros((clusters, 1), F32)
    for b in range(nz):
        is_mem = iota((clusters, rows), 0) == meta[b, 0:1, :]
        mem = is_mem.astype(F32)
        before = base + jnp.dot(mem.astype(BF16), tri, preferred_element_type=F32)

        def of_row(v):
            return jnp.sum(jnp.where(is_mem, v, 0.0), axis=0, keepdims=True)

        rank = of_row(before)
        vals = [of_row(place_c) + rank, rank + (q * seg).astype(F32), of_row(work_c),
                meta[b, 1:2, :].astype(F32) + 1.0, of_row(e_c) + 1.0]
        place[:, b * rows:(b + 1) * rows] = rows_of(vals, rows)
        base = base + jnp.sum(mem, axis=1, keepdims=True)

    all_rows = nz * rows
    place_i = place[0:1, :].astype(I32)
    label_row = iota((8, all_rows), 0)
    small = (label_row == 1) | (label_row == 3) | (label_row == 4)
    labels = jnp.where(small, place[...], 0.0).astype(BF16)

    def make_pick(t, _):
        hit = iota((slots, all_rows), 0) + t * slots == place_i
        pick[t] = jnp.where(hit, 1.0, 0.0).astype(BF16)
        ots[t] = lax.dot_general(labels, pick[t], (((1,), (1,)), ((), ())),
                                 preferred_element_type=F32)
        return 0

    lax.fori_loop(0, nq, make_pick, 0)
    otr[q] = ots[q]
    orders = [copy(ots.at[on_plane(d)], otr.at[q], s_ot.at[d], r_ot.at[d], z * nq + on_plane(d))
              for d in range(1, nq)]
    for c in orders:
        c.start()

    below = iota((half, CAP), 0) + half > iota((half, CAP), 1)

    def spread(k):
        for c in planes[k]:
            c.wait_recv()
        got = jnp.dot(repack[...].reshape(group * CAP, nq * slots),
                      plane[k].reshape(nq * slots, width), preferred_element_type=F32)
        units[...] = got.astype(BF16).reshape(group, CAP, width)

    def partial_gram(e):
        m = units[e]
        return lax.dot_general(m, m, (((1,), (1,)), ((), ())), preferred_element_type=F32)

    def add_gram(k):
        if k == 0:
            make_repack()
        spread(k)
        for e in range(group):
            s = partial_gram(e)
            gram[e] = s if k == 0 else gram[e] + s

    def make_repack():
        for c in orders:
            c.wait_recv()
        for t in range(nq):
            labs[:, t * slots:(t + 1) * slots] = otr[t]
        target = ((labs[4:5, :] - 1.0) * CAP + labs[1:2, :]).astype(I32)

        def one(e, _):
            hit = iota((CAP, nq * slots), 0) + e * CAP == target
            repack[e] = jnp.where(hit, 1.0, 0.0).astype(BF16)
            return 0

        lax.fori_loop(0, group, one, 0)

    planes = []
    for k in range(chunks):
        for c in lines[k]:
            c.wait_recv()
        block = line[k].reshape(all_rows, width)
        now = []
        for d in list(range(1, nq)) + [0]:
            t = on_plane(d)
            got = jnp.dot(pick[t], block, preferred_element_type=F32).astype(BF16)
            if d == 0:
                plane[k, q] = got
            else:
                packed[k, t] = got
                c = copy(packed.at[k, t], plane.at[k, q], s_plane.at[k, d], r_plane.at[k, d],
                         z * nq + t)
                c.start()
                now.append(c)
        planes.append(now)
        if k >= LAG:
            add_gram(k - LAG)

    for k in range(max(chunks - LAG, 0), chunks - 1):
        add_gram(k)
    if chunks == 1:
        make_repack()
    spread(chunks - 1)
    halves = []
    for d in list(range(1, nz)) + [0]:
        t = on_line(d)
        for l in range(per_owner):
            full = partial_gram(t * per_owner + l)
            if chunks > 1:
                full = full + gram[t * per_owner + l]
            hs[t, l] = jnp.where(below, full[half:, :], pltpu.roll(full[:half, :], half, 1))
        if d:
            c = copy(hs.at[t], hr.at[z], s_h.at[d], r_h.at[d], t * nq + q)
            c.start()
            halves.append(c)
    hr[z] = hs[z]
    ranks = labs[...].astype(BF16)
    ord_rows = []
    for l in range(per_owner):
        r = lax.dot_general(ranks, repack[z * per_owner + l], (((1,), (1,)), ((), ())),
                            preferred_element_type=F32)
        ord_rows.append(r[3:4, :])
    ord_r = rows_of(ord_rows, CAP)
    ord_cols = ord_r.T
    for c in halves:
        c.wait_recv()
    bests, means = [], []
    up = iota((half, half), 0) < iota((half, half), 1)
    down = iota((half, half), 0) > iota((half, half), 1)
    for l in range(per_owner):
        p = hr[0, l]
        for t in range(1, nz):
            p = p + hr[t, l]
        pt = p.T
        u, ut = p[:, half:], pt[half:, :]
        top = jnp.concatenate([jnp.where(up, u, ut), pt[:half, :]], axis=1)
        bottom = jnp.concatenate([p[:, :half], jnp.where(down, u, ut)], axis=1)
        sim = jnp.concatenate([top, bottom], axis=0)
        mine = (me * per_owner + l).astype(F32)
        n_mem = jnp.sum(jnp.where(work_c == mine, size_c, 0.0), axis=0, keepdims=True)
        o_row, o_col = ord_r[l:l + 1, :], ord_cols[:, l:l + 1]
        ok = (o_col < o_row) & (o_col >= 1.0) & (o_col <= n_mem)
        near = jnp.max(jnp.where(ok, sim, -1.0), axis=0, keepdims=True)
        live = (o_row >= 1.0) & (o_row <= n_mem)
        bests.append(jnp.where(live, near, -1.0))
        means.append(jnp.sum(jnp.where(live, near, 0.0), axis=1, keepdims=True) / n_mem)
    lanes = jnp.zeros((1, CAP), F32)
    for l in range(per_owner):
        lanes = jnp.where(iota((1, CAP), 1) == l, means[l], lanes)
    table[me] = rows_of(bests + [lanes], CAP)
    backs = [copy(table.at[me], table.at[me], s_t.at[d], r_t.at[d], lax.rem(me + d, n))
             for d in range(1, n)]
    for c in backs:
        c.start()
    own = pl.ds(pl.multiple_of(z * rows, rows), rows)
    s8 = place[2:3, own].astype(I32)
    pos = place[1:2, own].astype(I32)
    hot = jnp.where(iota((clusters, rows), 0) == s8, 1.0, 0.0)
    for c in backs:
        c.wait_recv()
    full = table[...]
    flat = full[:, :per_owner, :].reshape(clusters, CAP).T
    told = full[:, per_owner:per_owner + 1, :].reshape(n, CAP)
    mean = jnp.zeros((1, rows), F32)
    for l in range(per_owner):
        own_slot = (me * per_owner + l).astype(F32)
        work = jnp.sum(jnp.where(slot_c == own_slot, work_c, 0.0), axis=0, keepdims=True).astype(I32)
        hit = iota((n, CAP), 0) * per_owner + iota((n, CAP), 1) == work
        hit = hit & (iota((n, CAP), 1) < per_owner)
        part = jnp.sum(jnp.where(hit, told, 0.0), axis=1, keepdims=True)
        mean = jnp.where(iota((1, rows), 1) == l, jnp.sum(part, axis=0, keepdims=True), mean)
    got = jnp.dot(flat, hot, preferred_element_type=F32, precision=lax.Precision.HIGHEST)
    out = jnp.sum(jnp.where(iota((CAP, rows), 0) == pos, got, 0.0), axis=0, keepdims=True)
    packed_out[...] = rows_of([out, mean], rows)
    for group_of in [metas, orders, halves, backs] + lines + planes:
        for c in group_of:
            c.wait_send()


def finish(packed, best_out, keep_out, mean_out):
    best = packed[0:1, :]
    best_out[...] = best
    keep_out[...] = jnp.where(best < CUTOFF, 1, 0)
    mean_out[...] = packed[1:2, :mean_out.shape[1]]


def body(embeddings, cluster_id, member_order, cluster_slot, cluster_size):
    n = lax.axis_size("dev")
    nz, nq = split_lines(n)
    rows, depth = embeddings.shape
    clusters = cluster_slot.shape[0]
    per_owner = clusters // n
    width = min(CHUNK, depth // nz)
    chunks = depth // nz // width
    group = nz * per_owner
    slots = line_slots(n, nz, nq, rows, group)
    vmem = pl.BlockSpec(memory_space=pltpu.VMEM)
    dma = pltpu.SemaphoreType.DMA
    packed = pl.pallas_call(
        functools.partial(kernel, n, nz, nq),
        out_shape=jax.ShapeDtypeStruct((8, rows), F32),
        in_specs=[pl.BlockSpec(memory_space=pl.ANY)] + [vmem] * 4,
        out_specs=vmem,
        scratch_shapes=[
            pltpu.VMEM((rows, depth), F32),
            dma((LOADS,)),
            pltpu.VMEM((nz, chunks, rows, width), BF16),
            pltpu.VMEM((chunks, nz, rows, width), BF16),
            pltpu.VMEM((nz, 8, rows), I32),
            pltpu.VMEM((8, nz * rows), F32),
            pltpu.VMEM((nq, slots, nz * rows), BF16),
            pltpu.VMEM((chunks, nq, slots, width), BF16),
            pltpu.VMEM((chunks, nq, slots, width), BF16),
            pltpu.VMEM((nq, 8, slots), F32),
            pltpu.VMEM((nq, 8, slots), F32),
            pltpu.VMEM((group, CAP, CAP), F32),
            pltpu.VMEM((nz, per_owner, CAP // 2, CAP), F32),
            pltpu.VMEM((nz, per_owner, CAP // 2, CAP), F32),
            pltpu.VMEM((n, 8, CAP), F32),
            pltpu.VMEM((group, CAP, width), BF16),
            pltpu.VMEM((group, CAP, nq * slots), BF16),
            pltpu.VMEM((8, nq * slots), F32),
            dma((nz,)), dma((nz,)),
            dma((chunks, nz)), dma((chunks, nz)),
            dma((chunks, nq)), dma((chunks, nq)),
            dma((nq,)), dma((nq,)),
            dma((nz,)), dma((nz,)),
            dma((n,)), dma((n,)),
        ],
        compiler_params=pltpu.CompilerParams(
            collective_id=0, has_side_effects=True, vmem_limit_bytes=60 * 1024 * 1024),
    )(embeddings, cluster_id.reshape(1, rows), member_order.reshape(1, rows),
      cluster_slot.reshape(1, clusters), cluster_size.reshape(1, clusters))
    best, keep, mean = pl.pallas_call(
        finish,
        out_shape=(jax.ShapeDtypeStruct((1, rows), F32), jax.ShapeDtypeStruct((1, rows), I32),
                   jax.ShapeDtypeStruct((1, per_owner), F32)),
        in_specs=[vmem],
        out_specs=(vmem,) * 3,
    )(packed)
    return best.reshape(rows), keep.reshape(rows), mean.reshape(per_owner)


def solution(mesh):
    placed = (P(("rep", "dev"), None), P(("rep", "dev")), P(("rep", "dev")), P("rep"), P("rep"))
    return jax.shard_map(
        body,
        mesh=mesh,
        in_specs=placed,
        out_specs=(P(("rep", "dev")), P(("rep", "dev")), P(("rep", "dev"))),
        check_vma=False,
    )
```

```python
import functools

import jax
import jax.numpy as jnp
from jax import lax
from jax.experimental import pallas as pl
from jax.experimental.pallas import tpu as pltpu
from jax.sharding import PartitionSpec as P

CAP = 128
CHUNK = 128
LOADS = 4
LAG = 2
NORM_EPS = 1e-06
CUTOFF = 0.8
F32 = jnp.float32
BF16 = jnp.bfloat16
I32 = jnp.int32


def split_lines(n):
    z = max(z for z in range(1, n + 1) if n % z == 0 and z * z <= n)
    return z, n // z


def line_slots(n, nz, nq, rows, group):
    largest = rows * n // nq + CAP - CAP // nq
    bound = -(-largest // nq) + -(-group * nz * (n - 1) // n)
    return min(group * (CAP // nq), -(-bound // 16) * 16)


def iota(shape, dim):
    return lax.broadcasted_iota(I32, shape, dim)


def rows_of(values, width):
    row = iota((8, width), 0)
    out = jnp.zeros((8, width), values[0].dtype)
    for r, v in enumerate(values):
        out = jnp.where(row == r, jnp.broadcast_to(v, (8, width)), out)
    return out


def to_col(row, count):
    eye = iota((count, count), 0) == iota((count, count), 1)
    return jnp.sum(jnp.where(eye, row, 0.0), axis=1, keepdims=True)


def floor_div(x, d):
    return jnp.floor((x + 0.5) * (1.0 / d))


def kernel(n, nz, nq, emb_hbm, cid, order, slot, size, packed_out,
           emb, s_load, unit, line, meta, place, pick, packed, plane, ots, otr, gram, hs, hr, table, units, repack, labs,
           s_meta, r_meta, s_line, r_line, s_plane, r_plane, s_ot, r_ot, s_h, r_h, s_t, r_t):
    me = lax.axis_index("dev")
    parts = s_load.shape[0]
    tall = emb.shape[0] // parts
    loads = [pltpu.make_async_copy(emb_hbm.at[pl.ds(i * tall, tall)], emb.at[pl.ds(i * tall, tall)],
                                   s_load.at[i]) for i in range(parts)]
    for c in loads:
        c.start()
    z, q = lax.div(me, nq), lax.rem(me, nq)
    rows = emb.shape[0]
    clusters = slot.shape[1]
    per_owner = clusters // n
    chunks, width = unit.shape[1], unit.shape[3]
    group = nz * per_owner
    seg = CAP // nq
    slots = pick.shape[1]
    half = CAP // 2

    def copy(src, dst, s, r, target):
        return pltpu.make_async_remote_copy(
            src_ref=src, dst_ref=dst, send_sem=s, recv_sem=r,
            device_id={"dev": target}, device_id_type=pl.DeviceIdType.MESH)

    def on_line(d):
        return lax.rem(z + d, nz)

    def on_plane(d):
        return lax.rem(q + d, nq)

    barrier = pltpu.get_barrier_semaphore()
    friends = [on_line(d) * nq + q for d in range(1, nz)] + [z * nq + on_plane(d) for d in range(1, nq)]
    for t in friends:
        pl.semaphore_signal(barrier, inc=1, device_id={"dev": t},
                            device_id_type=pl.DeviceIdType.MESH)

    meta[z] = rows_of([cid[...], order[...]], rows)
    sums = []
    for i in range(parts):
        loads[i].wait()
        x = emb[i * tall:(i + 1) * tall, :]
        sums.append(jnp.sum(x * x, axis=1, keepdims=True))
    scale = lax.rsqrt(jnp.concatenate(sums, axis=0) + NORM_EPS)
    pl.semaphore_wait(barrier, len(friends))

    metas = [copy(meta.at[z], meta.at[z], s_meta.at[d], r_meta.at[d], on_line(d) * nq + q)
             for d in range(1, nz)]
    for c in metas:
        c.start()
    lines = []
    for k in range(chunks):
        for t in range(nz):
            c0 = (t * chunks + k) * width
            unit[t, k] = (emb[:, c0:c0 + width] * scale).astype(BF16)
        now = [copy(unit.at[on_line(d), k], line.at[k, z], s_line.at[k, d], r_line.at[k, d],
                    on_line(d) * nq + q) for d in range(nz - 1, 0, -1)]
        for c in now:
            c.start()
        line[k, z] = unit[z, k]
        lines.append(now)

    slot_c = to_col(slot[...].astype(F32), clusters)
    size_c = to_col(size[...].astype(F32), clusters)
    size_r = size[...].astype(F32)
    c_row, c_col = iota((clusters, clusters), 1), iota((clusters, clusters), 0)
    ahead = (size_r > size_c) | ((size_r == size_c) & (c_row < c_col))
    place_in = jnp.sum(jnp.where(ahead, 1.0, 0.0), axis=1, keepdims=True)
    e_c = floor_div(place_in, nq)
    turn = place_in - e_c * nq
    odd = e_c - 2.0 * floor_div(e_c, 2)
    g_c = jnp.where(odd > 0.5, nq - 1 - turn, turn)
    oz_c = floor_div(e_c, per_owner)
    local_c = e_c - oz_c * per_owner
    work_c = (oz_c * nq + g_c) * per_owner + local_c
    for c in metas:
        c.wait_recv()
    tri = (iota((rows, rows), 0) < iota((rows, rows), 1)).astype(F32).astype(BF16)
    counts = jnp.zeros((clusters, 1), F32)
    for b in range(nz):
        mem = jnp.where(iota((clusters, rows), 0) == meta[b, 0:1, :], 1.0, 0.0)
        counts = counts + jnp.sum(mem, axis=1, keepdims=True)
    eye = c_row == c_col
    g_r = jnp.sum(jnp.where(eye, g_c, 0.0), axis=0, keepdims=True)
    e_r = jnp.sum(jnp.where(eye, e_c, 0.0), axis=0, keepdims=True)
    n_r = jnp.sum(jnp.where(eye, counts, 0.0), axis=0, keepdims=True)
    first = (g_r == g_c) & (e_r < e_c)
    place_c = g_c * slots + jnp.sum(jnp.where(first, n_r, 0.0), axis=1, keepdims=True)
    base = jnp.zeros((clusters, 1), F32)
    for b in range(nz):
        is_mem = iota((clusters, rows), 0) == meta[b, 0:1, :]
        mem = is_mem.astype(F32)
        before = base + jnp.dot(mem.astype(BF16), tri, preferred_element_type=F32)

        def of_row(v):
            return jnp.sum(jnp.where(is_mem, v, 0.0), axis=0, keepdims=True)

        rank = of_row(before)
        vals = [of_row(place_c) + rank, rank + (q * seg).astype(F32), of_row(work_c),
                meta[b, 1:2, :].astype(F32) + 1.0, of_row(e_c) + 1.0]
        place[:, b * rows:(b + 1) * rows] = rows_of(vals, rows)
        base = base + jnp.sum(mem, axis=1, keepdims=True)

    all_rows = nz * rows
    place_i = place[0:1, :].astype(I32)
    label_row = iota((8, all_rows), 0)
    small = (label_row == 1) | (label_row == 3) | (label_row == 4)
    labels = jnp.where(small, place[...], 0.0).astype(BF16)

    def make_pick(t, _):
        hit = iota((slots, all_rows), 0) + t * slots == place_i
        pick[t] = jnp.where(hit, 1.0, 0.0).astype(BF16)
        ots[t] = lax.dot_general(labels, pick[t], (((1,), (1,)), ((), ())),
                                 preferred_element_type=F32)
        return 0

    lax.fori_loop(0, nq, make_pick, 0)
    otr[q] = ots[q]
    orders = [copy(ots.at[on_plane(d)], otr.at[q], s_ot.at[d], r_ot.at[d], z * nq + on_plane(d))
              for d in range(1, nq)]
    for c in orders:
        c.start()

    below = iota((half, CAP), 0) + half > iota((half, CAP), 1)

    def spread(k):
        for c in planes[k]:
            c.wait_recv()
        got = jnp.dot(repack[...].reshape(group * CAP, nq * slots),
                      plane[k].reshape(nq * slots, width), preferred_element_type=F32)
        units[...] = got.astype(BF16).reshape(group, CAP, width)

    def partial_gram(e):
        m = units[e]
        return lax.dot_general(m, m, (((1,), (1,)), ((), ())), preferred_element_type=F32)

    def add_gram(k):
        if k == 0:
            make_repack()
        spread(k)
        for e in range(group):
            s = partial_gram(e)
            gram[e] = s if k == 0 else gram[e] + s

    def make_repack():
        for c in orders:
            c.wait_recv()
        for t in range(nq):
            labs[:, t * slots:(t + 1) * slots] = otr[t]
        target = ((labs[4:5, :] - 1.0) * CAP + labs[1:2, :]).astype(I32)

        def one(e, _):
            hit = iota((CAP, nq * slots), 0) + e * CAP == target
            repack[e] = jnp.where(hit, 1.0, 0.0).astype(BF16)
            return 0

        lax.fori_loop(0, group, one, 0)

    planes = []
    for k in range(chunks):
        for c in lines[k]:
            c.wait_recv()
        block = line[k].reshape(all_rows, width)
        now = []
        for d in list(range(1, nq)) + [0]:
            t = on_plane(d)
            got = jnp.dot(pick[t], block, preferred_element_type=F32).astype(BF16)
            if d == 0:
                plane[k, q] = got
            else:
                packed[k, t] = got
                c = copy(packed.at[k, t], plane.at[k, q], s_plane.at[k, d], r_plane.at[k, d],
                         z * nq + t)
                c.start()
                now.append(c)
        planes.append(now)
        if k >= LAG:
            add_gram(k - LAG)

    for k in range(max(chunks - LAG, 0), chunks - 1):
        add_gram(k)
    if chunks == 1:
        make_repack()
    spread(chunks - 1)
    halves = []
    for d in list(range(1, nz)) + [0]:
        t = on_line(d)
        for l in range(per_owner):
            full = partial_gram(t * per_owner + l)
            if chunks > 1:
                full = full + gram[t * per_owner + l]
            hs[t, l] = jnp.where(below, full[half:, :], pltpu.roll(full[:half, :], half, 1))
        if d:
            c = copy(hs.at[t], hr.at[z], s_h.at[d], r_h.at[d], t * nq + q)
            c.start()
            halves.append(c)
    hr[z] = hs[z]
    ranks = labs[...].astype(BF16)
    ord_rows = []
    for l in range(per_owner):
        r = lax.dot_general(ranks, repack[z * per_owner + l], (((1,), (1,)), ((), ())),
                            preferred_element_type=F32)
        ord_rows.append(r[3:4, :])
    ord_r = rows_of(ord_rows, CAP)
    ord_cols = ord_r.T
    for c in halves:
        c.wait_recv()
    bests, means = [], []
    up = iota((half, half), 0) < iota((half, half), 1)
    down = iota((half, half), 0) > iota((half, half), 1)
    for l in range(per_owner):
        p = hr[0, l]
        for t in range(1, nz):
            p = p + hr[t, l]
        pt = p.T
        u, ut = p[:, half:], pt[half:, :]
        top = jnp.concatenate([jnp.where(up, u, ut), pt[:half, :]], axis=1)
        bottom = jnp.concatenate([p[:, :half], jnp.where(down, u, ut)], axis=1)
        sim = jnp.concatenate([top, bottom], axis=0)
        mine = (me * per_owner + l).astype(F32)
        n_mem = jnp.sum(jnp.where(work_c == mine, size_c, 0.0), axis=0, keepdims=True)
        o_row, o_col = ord_r[l:l + 1, :], ord_cols[:, l:l + 1]
        ok = (o_col < o_row) & (o_col >= 1.0) & (o_col <= n_mem)
        near = jnp.max(jnp.where(ok, sim, -1.0), axis=0, keepdims=True)
        live = (o_row >= 1.0) & (o_row <= n_mem)
        bests.append(jnp.where(live, near, -1.0))
        means.append(jnp.sum(jnp.where(live, near, 0.0), axis=1, keepdims=True) / n_mem)
    lanes = jnp.zeros((1, CAP), F32)
    for l in range(per_owner):
        lanes = jnp.where(iota((1, CAP), 1) == l, means[l], lanes)
    table[me] = rows_of(bests + [lanes], CAP)[:table.shape[1], :]
    backs = [copy(table.at[me], table.at[me], s_t.at[d], r_t.at[d], lax.rem(me + d, n))
             for d in range(1, n)]
    for c in backs:
        c.start()
    own = pl.ds(pl.multiple_of(z * rows, rows), rows)
    s8 = place[2:3, own].astype(I32)
    pos = place[1:2, own].astype(I32)
    hot = jnp.where(iota((clusters, rows), 0) == s8, 1.0, 0.0)
    for c in backs:
        c.wait_recv()
    full = table[...]
    flat = full[:, :per_owner, :].reshape(clusters, CAP).T
    told = full[:, per_owner:per_owner + 1, :].reshape(n, CAP)
    mean = jnp.zeros((1, rows), F32)
    for l in range(per_owner):
        own_slot = (me * per_owner + l).astype(F32)
        work = jnp.sum(jnp.where(slot_c == own_slot, work_c, 0.0), axis=0, keepdims=True).astype(I32)
        hit = iota((n, CAP), 0) * per_owner + iota((n, CAP), 1) == work
        hit = hit & (iota((n, CAP), 1) < per_owner)
        part = jnp.sum(jnp.where(hit, told, 0.0), axis=1, keepdims=True)
        mean = jnp.where(iota((1, rows), 1) == l, jnp.sum(part, axis=0, keepdims=True), mean)
    got = jnp.dot(flat, hot, preferred_element_type=F32, precision=lax.Precision.HIGHEST)
    out = jnp.sum(jnp.where(iota((CAP, rows), 0) == pos, got, 0.0), axis=0, keepdims=True)
    packed_out[...] = rows_of([out, mean], rows)
    for group_of in [metas, orders, halves, backs] + lines + planes:
        for c in group_of:
            c.wait_send()


def finish(packed, best_out, keep_out, mean_out):
    best = packed[0:1, :]
    best_out[...] = best
    keep_out[...] = jnp.where(best < CUTOFF, 1, 0)
    mean_out[...] = packed[1:2, :mean_out.shape[1]]


def body(embeddings, cluster_id, member_order, cluster_slot, cluster_size):
    n = lax.axis_size("dev")
    nz, nq = split_lines(n)
    rows, depth = embeddings.shape
    clusters = cluster_slot.shape[0]
    per_owner = clusters // n
    width = min(CHUNK, depth // nz)
    chunks = depth // nz // width
    group = nz * per_owner
    slots = line_slots(n, nz, nq, rows, group)
    vmem = pl.BlockSpec(memory_space=pltpu.VMEM)
    dma = pltpu.SemaphoreType.DMA
    packed = pl.pallas_call(
        functools.partial(kernel, n, nz, nq),
        out_shape=jax.ShapeDtypeStruct((8, rows), F32),
        in_specs=[pl.BlockSpec(memory_space=pl.ANY)] + [vmem] * 4,
        out_specs=vmem,
        scratch_shapes=[
            pltpu.VMEM((rows, depth), F32),
            dma((LOADS,)),
            pltpu.VMEM((nz, chunks, rows, width), BF16),
            pltpu.VMEM((chunks, nz, rows, width), BF16),
            pltpu.VMEM((nz, 8, rows), I32),
            pltpu.VMEM((8, nz * rows), F32),
            pltpu.VMEM((nq, slots, nz * rows), BF16),
            pltpu.VMEM((chunks, nq, slots, width), BF16),
            pltpu.VMEM((chunks, nq, slots, width), BF16),
            pltpu.VMEM((nq, 8, slots), F32),
            pltpu.VMEM((nq, 8, slots), F32),
            pltpu.VMEM((group, CAP, CAP), F32),
            pltpu.VMEM((nz, per_owner, CAP // 2, CAP), F32),
            pltpu.VMEM((nz, per_owner, CAP // 2, CAP), F32),
            pltpu.VMEM((n, pl.next_power_of_2(per_owner + 1), CAP), F32),
            pltpu.VMEM((group, CAP, width), BF16),
            pltpu.VMEM((group, CAP, nq * slots), BF16),
            pltpu.VMEM((8, nq * slots), F32),
            dma((nz,)), dma((nz,)),
            dma((chunks, nz)), dma((chunks, nz)),
            dma((chunks, nq)), dma((chunks, nq)),
            dma((nq,)), dma((nq,)),
            dma((nz,)), dma((nz,)),
            dma((n,)), dma((n,)),
        ],
        compiler_params=pltpu.CompilerParams(
            collective_id=0, has_side_effects=True, vmem_limit_bytes=60 * 1024 * 1024),
    )(embeddings, cluster_id.reshape(1, rows), member_order.reshape(1, rows),
      cluster_slot.reshape(1, clusters), cluster_size.reshape(1, clusters))
    best, keep, mean = pl.pallas_call(
        finish,
        out_shape=(jax.ShapeDtypeStruct((1, rows), F32), jax.ShapeDtypeStruct((1, rows), I32),
                   jax.ShapeDtypeStruct((1, per_owner), F32)),
        in_specs=[vmem],
        out_specs=(vmem,) * 3,
    )(packed)
    return best.reshape(rows), keep.reshape(rows), mean.reshape(per_owner)


def solution(mesh):
    placed = (P(("rep", "dev"), None), P(("rep", "dev")), P(("rep", "dev")), P("rep"), P("rep"))
    return jax.shard_map(
        body,
        mesh=mesh,
        in_specs=placed,
        out_specs=(P(("rep", "dev")), P(("rep", "dev")), P(("rep", "dev"))),
        check_vma=False,
    )
```
